32 devices in a mesh: sta: 16 (over z, x, core), tpl: 2 (over y).
Axes of the slice: x: 2, y: 2, z: 4, core: 2. Of those that a mesh axis runs over, the one named last changes fastest.
Arguments:
- waveform: bfloat16 [16, 3, 4279], P('sta'), may hold values from -150 to 150
- templates: bfloat16 [128, 16, 1536], P('tpl', 'sta'), may hold values from -6 to 6
- lags: int32 [128, 16], P('tpl', 'sta'), may hold values from 0 to 3000
- present: int32 [128, 16], P('tpl', 'sta'), may hold values 0 or 1
Outputs:
- score: float32 [768, 128], P('sta', 'tpl')
- scale_mad: float32 [128], P('tpl')
- peak: float32 [768], P('sta')
The draws below stay inside these ranges and needn't reach their ends.
All inputs are finite; a program needn't handle non-finite values. No bound on the sum of `present` on one device may be relied on, other than what follows from the above.
Results may differ from the reference program's by a relative error of at most 0.0003.
Values may be sent and summed in bfloat16 or wider, within the bound.
No kernel may reach another device: no remote copies, remote signals or barrier semaphores. Data moves between devices by JAX's collectives and lax.ppermute only.
A program may use at most 64 MiB of HBM per device.

```python
import jax
import jax.numpy as jnp
from jax import lax

LEN = 512
CHANS = 3
LAG = 3000
BINS = 1024
STATIONS = 16
TEMPLATES = 128
TOUT = 768
SAMPLES = 4279


def draw_waveform(key, part):
    key_noise = jax.random.fold_in(key, 11)
    key_scale = jax.random.fold_in(key, 12)
    timeline = jnp.arange(SAMPLES, dtype=jnp.float32) / SAMPLES
    envelope = jnp.exp(jnp.log(3.0) * timeline)
    noise = jnp.clip(jax.random.normal(key_noise, (STATIONS, 3, SAMPLES), jnp.float32), -5.0, 5.0)
    scales = jnp.exp(jax.random.uniform(key_scale, (STATIONS, 1, 1), jnp.float32, 0.0, jnp.log(10.0)))
    return (noise * scales * envelope).astype(jnp.bfloat16)


def touch_ends(drawn, own_key, smallest, top_value):
    longest = drawn.shape.index(max(drawn.shape))
    spots = []
    for shift in (0, 1):
        where = [jax.random.randint(jax.random.fold_in(own_key, axis), (), 0, length) for axis, length in enumerate(drawn.shape)]
        where[longest] = (where[longest] + shift) % drawn.shape[longest]
        spots.append(tuple(where))
    return drawn.at[spots[0]].set(smallest).at[spots[1]].set(top_value)


def shard_levels(own_key, extent, shards, least, high):
    loudness, own = 1.0, jax.random.fold_in(own_key, 6)
    for axis_at, blocks in shards:
        draws = jnp.exp(jax.random.uniform(jax.random.fold_in(own, axis_at), (blocks,), jnp.float32, least / len(shards), high / len(shards)))
        loudness = loudness * jnp.repeat(draws, extent[axis_at] // blocks).reshape([-1 if axis == axis_at else 1 for axis in range(len(extent))])
    return loudness


def normal_values(own_key, extent, scale, most, pieces=(), held_as=jnp.bfloat16):
    values = scale * jax.random.normal(own_key, extent, jnp.float32)
    if pieces:
        values = values * shard_levels(own_key, extent, pieces, -0.22, 0.18)
    return jnp.clip(values, -most, most).astype(held_as)


def setup_inputs(seed: int = 0) -> dict:
    streams_of = jax.random.split(jax.random.key(seed), 5)
    waveform = draw_waveform(jax.random.fold_in(streams_of[4], 71), 0)
    templates = normal_values(streams_of[1], (TEMPLATES, STATIONS, CHANS * LEN), 1.0, 6.0, ((0, 2), (1, 16)))
    lags = touch_ends(jax.random.randint(streams_of[2], (TEMPLATES, STATIONS), 0, LAG + 1), jax.random.fold_in(streams_of[2], 1), 0, LAG).astype(jnp.int32)
    present = touch_ends((jax.random.randint(streams_of[3], (TEMPLATES, STATIONS), 0, 4) < 3).astype(jnp.int32), jax.random.fold_in(streams_of[3], 1), 0, 1)
    return dict(waveform=waveform, templates=templates, lags=lags, present=present)


def toeplitz_rows(record, length, columns):
    count = record.shape[1]
    chans = record.shape[0]
    tiled = jnp.broadcast_to(record[:, None, :], (chans, length + 1, count))
    tiled = tiled.reshape(chans, (length + 1) * count)[:, :length * (count + 1)]
    tiled = tiled.reshape(chans, length, count + 1)[:, :, :columns]
    return tiled.reshape(chans * length, columns)

def shift_rows(block, offsets, count):
    return jax.vmap(lambda row, offset: lax.dynamic_slice_in_dim(row, offset, count))(block, offsets.astype(jnp.int32))

def hat_counts(values, nbins):
    width = 512.0 / nbins
    ncols = values.shape[1]
    position = jnp.clip(jnp.abs(values) / width - 0.5, 0.0, nbins - 1.0)
    lower = jnp.minimum(jnp.floor(position), nbins - 2.0)
    weight = position - lower
    index = lower.astype(jnp.int32) + nbins * jnp.arange(ncols, dtype=jnp.int32)[None, :]
    flat_index = index.reshape(-1)
    flat_weight = weight.reshape(-1)
    counts = jax.ops.segment_sum(1.0 - flat_weight, flat_index, num_segments=ncols * nbins)
    counts = counts + jax.ops.segment_sum(flat_weight, flat_index + 1, num_segments=ncols * nbins)
    return counts.reshape(ncols, nbins)

def median_abs(counts, halfway):
    width = 512.0 / counts.shape[1]
    running = jnp.cumsum(counts, axis=1)
    earlier = running - counts
    share = jnp.clip((halfway - earlier) / jnp.maximum(counts, 1.0), 0.0, 1.0)
    return width * lax.optimization_barrier(jnp.sum(share, axis=1))

def reference(waveform, templates, lags, present):
    total = TOUT
    span = TOUT + LAG
    tnorm = jnp.sqrt(lax.optimization_barrier(jnp.sum(templates.astype(jnp.float32) ** 2, axis=2)) + 1e-06)

    def station(stack, items):
        record, pattern, offsets, member, scaling = items
        columns = toeplitz_rows(record, LEN, span)
        corr = jnp.dot(pattern, columns, preferred_element_type=jnp.float32) / scaling[:, None]
        moved = shift_rows(corr, offsets, total) * member[:, None].astype(jnp.float32)
        return (stack + moved, None)
    start = jnp.zeros((templates.shape[0], total), jnp.float32)
    stack, unused = lax.scan(station, start, (waveform, jnp.swapaxes(templates, 0, 1), lags.T, present.T, tnorm.T))
    stack = stack.T
    counts = hat_counts(stack, BINS)
    median = median_abs(counts, 0.5 * total)
    scale_mad = 1.4826 * median
    score = stack / scale_mad[None, :]
    peak = lax.optimization_barrier(jnp.max(score, axis=1))
    return (score, scale_mad, peak)
```

```python
import jax
import jax.numpy as jnp
from jax import lax
from jax.experimental import pallas as pl
from jax.experimental.pallas import tpu as pltpu
from jax.sharding import PartitionSpec as P

LEN = 512
LAG = 3000
BINS = 1024
TOUT_DEV = 48
LANES = 128
TILE = 256


def ceil_to(value, step):
    return -(-value // step) * step


def correlate(waveform, pattern, offsets, present, total):
    chans, samples = waveform.shape[1:]
    ntpl, width = pattern.shape
    taps = LEN // LANES
    rows = total // LANES
    fetch = ceil_to(rows + 1, 8)
    columns = ceil_to(total + LAG, TILE)
    held = ceil_to(max(LAG // LANES + fetch, columns // LANES), 8)
    built = columns + LEN - LANES
    padded = ceil_to(max(built + LANES, samples), LANES)

    def kernel(lag_ref, wave_ref, pattern_ref, present_ref, out_ref, line_ref, hankel_ref, corr_ref):
        line_ref[...] = jnp.zeros_like(line_ref)
        line_ref[0:chans, 0:samples] = wave_ref[0].astype(jnp.float32)
        pattern_in = pattern_ref[...]
        wide = pattern_in.astype(jnp.float32)
        tnorm = jnp.sqrt(jnp.sum(wide * wide, axis=1, keepdims=True) + 1e-06)
        factor = present_ref[...].astype(jnp.float32) / tnorm
        step = lax.broadcasted_iota(jnp.int32, (8, padded), 0)
        for c in range(chans):
            base = jnp.broadcast_to(line_ref[c : c + 1, :], (8, padded))
            for k in (1, 2, 4):
                base = jnp.where((step & k) != 0, pltpu.roll(base, padded - k, 1), base)
            for h in range(LANES // 16):
                low = base if h == 0 else pltpu.roll(base, padded - 16 * h, 1)
                high = pltpu.roll(base, padded - 16 * h - 8, 1)
                both = jnp.concatenate([low, high], axis=0).astype(jnp.bfloat16)
                hankel_ref[c, 16 * h : 16 * h + 16, :] = both[:, :built]
        for n in range(columns // TILE):
            right = jnp.concatenate(
                [
                    hankel_ref[c, :, n * TILE + a * LANES : n * TILE + a * LANES + TILE]
                    for c in range(chans)
                    for a in range(taps)
                ],
                axis=0,
            )
            corr = jnp.dot(pattern_in, right, preferred_element_type=jnp.float32) * factor
            for part in range(TILE // LANES):
                place = n * (TILE // LANES) + part
                corr_ref[pl.ds(place, ntpl, stride=held), :] = corr[:, part * LANES : (part + 1) * LANES]
        lane = lax.broadcasted_iota(jnp.int32, (fetch, LANES), 1)
        for t in range(ntpl):
            lag = lag_ref[t]
            block = lag // LANES
            rest = lag - block * LANES
            got = corr_ref[pl.ds(t * held + block, fetch), :]
            turned = pltpu.roll(got, LANES - rest, 1)
            below = pltpu.roll(turned, fetch - 1, 0)
            moved = jnp.where(lane < LANES - rest, turned, below)
            out_ref[t * rows : (t + 1) * rows, :] = moved[0:rows, :]

    return pl.pallas_call(
        kernel,
        out_shape=jax.ShapeDtypeStruct((ntpl * rows, LANES), jnp.float32),
        in_specs=[
            pl.BlockSpec(memory_space=pltpu.SMEM),
            pl.BlockSpec(memory_space=pltpu.VMEM),
            pl.BlockSpec(memory_space=pltpu.VMEM),
            pl.BlockSpec(memory_space=pltpu.VMEM),
        ],
        out_specs=pl.BlockSpec(memory_space=pltpu.VMEM),
        scratch_shapes=[
            pltpu.VMEM((8, padded), jnp.float32),
            pltpu.VMEM((chans, LANES, built), jnp.bfloat16),
            pltpu.VMEM((ntpl * held, LANES), jnp.float32),
        ],
        name="correlate",
    )(offsets, waveform, pattern, present)


def score_rows(arrived, stations, groups, total):
    rows = total // LANES
    count = arrived.shape[0] // stations
    ntpl = count // rows
    width = 512.0 / BINS

    def kernel(in_ref, out_ref, stack_ref):
        stack = in_ref[0:count, :]
        for s in range(1, stations):
            stack = stack + in_ref[s * count : (s + 1) * count, :]
        stack_ref[...] = stack
        position = jnp.clip(jnp.abs(stack) / width - 0.5, 0.0, BINS - 1.0)
        fill = jnp.zeros((LANES - count, LANES), jnp.float32)
        turned = jnp.transpose(jnp.concatenate([position, fill], axis=0))
        bins = lax.broadcasted_iota(jnp.int32, (8, BINS), 1).astype(jnp.float32)
        sums = []
        for t in range(ntpl):
            acc = jnp.zeros((8, BINS), jnp.float32)
            for m in range(rows):
                for r in range(LANES // 8):
                    at = t * rows + m
                    spot = turned[8 * r : 8 * r + 8, at : at + 1]
                    acc = acc + jnp.clip(bins - spot, 0.0, 1.0)
            sums.append(jnp.sum(acc, axis=0, keepdims=True))
        before = jnp.concatenate(sums, axis=0) if ntpl > 1 else sums[0]
        last = lax.broadcasted_iota(jnp.int32, before.shape, 1) == BINS - 1
        cum = jnp.where(last, float(total), pltpu.roll(before, BINS - 1, 1))
        share = jnp.clip((0.5 * total - before) / jnp.maximum(cum - before, 1.0), 0.0, 1.0)
        scale = 1.4826 * (width * jnp.sum(share, axis=1, keepdims=True))
        score = jnp.concatenate(
            [stack_ref[pl.ds(m, ntpl, stride=rows), :] for m in range(rows)], axis=1
        ) / scale
        best = jnp.broadcast_to(jnp.max(score, axis=0, keepdims=True), score.shape)
        lane = lax.broadcasted_iota(jnp.int32, (ntpl, LANES), 1)
        for i in range(stations):
            begin = i * TOUT_DEV
            mine = score if begin == 0 else pltpu.roll(score, total - begin, 1)
            tops = pltpu.roll(best, (total + TOUT_DEV - begin) % total, 1)
            block = jnp.where(lane < TOUT_DEV, mine[:, :LANES], tops[:, :LANES])
            block = jnp.where(lane < 2 * TOUT_DEV, block, scale)
            for g in range(groups):
                place = (i * groups + g) * ntpl
                out_ref[place : place + ntpl, :] = block

    return pl.pallas_call(
        kernel,
        out_shape=jax.ShapeDtypeStruct((stations * groups * ntpl, LANES), jnp.float32),
        in_specs=[pl.BlockSpec(memory_space=pltpu.VMEM)],
        out_specs=pl.BlockSpec(memory_space=pltpu.VMEM),
        scratch_shapes=[pltpu.VMEM((count, LANES), jnp.float32)],
        name="scores",
    )(arrived)


def finish(arrived, group, stations, groups):
    ntpl = arrived.shape[0] // (stations * groups)
    held = stations * ntpl

    def kernel(group_ref, in_ref, score_ref, scale_ref, peak_ref, mine_ref):
        own = group_ref[0]
        for t in range(ntpl):
            mine_ref[pl.ds(t, stations, stride=ntpl), :] = in_ref[
                pl.ds(own * ntpl + t, stations, stride=groups * ntpl), :
            ]
        mine = mine_ref[...]
        if held < LANES:
            mine = jnp.concatenate([mine, jnp.zeros((LANES - held, LANES), jnp.float32)], axis=0)
        turned = jnp.transpose(mine)
        score_ref[...] = turned[0:TOUT_DEV, 0:held]
        scale_ref[...] = turned[2 * TOUT_DEV : 2 * TOUT_DEV + 1, 0:held]
        best = jnp.max(in_ref[...], axis=0, keepdims=True)
        peak_ref[...] = pltpu.roll(jnp.broadcast_to(best, (8, LANES)), LANES - TOUT_DEV, 1)[0:1, 0:TOUT_DEV]

    return pl.pallas_call(
        kernel,
        out_shape=(
            jax.ShapeDtypeStruct((TOUT_DEV, held), jnp.float32),
            jax.ShapeDtypeStruct((1, held), jnp.float32),
            jax.ShapeDtypeStruct((1, TOUT_DEV), jnp.float32),
        ),
        in_specs=[pl.BlockSpec(memory_space=pltpu.SMEM), pl.BlockSpec(memory_space=pltpu.VMEM)],
        out_specs=(pl.BlockSpec(memory_space=pltpu.VMEM),) * 3,
        scratch_shapes=[pltpu.VMEM((held, LANES), jnp.float32)],
        name="finish",
    )(group, arrived)


def on_device(waveform, templates, lags, present):
    stations = lax.axis_size("sta")
    groups = lax.axis_size("tpl")
    total = TOUT_DEV * stations
    moved = correlate(waveform, templates[:, 0, :], lags[:, 0], present, total)
    arrived = lax.all_to_all(moved, "sta", split_axis=0, concat_axis=0, tiled=True)
    scored = score_rows(arrived, stations, groups, total)
    spread = lax.all_to_all(scored, ("sta", "tpl"), split_axis=0, concat_axis=0, tiled=True)
    group = lax.axis_index("tpl").astype(jnp.int32).reshape(1)
    score, scale_mad, peak = finish(spread, group, stations, groups)
    return (score, scale_mad.reshape(-1), peak.reshape(-1))


def solution(mesh):
    placed = (P("sta", None, None), P("tpl", "sta", None), P("tpl", "sta"), P("tpl", "sta"))
    return jax.shard_map(
        on_device,
        mesh=mesh,
        in_specs=placed,
        out_specs=(P("sta", "tpl"), P("tpl"), P("sta")),
        check_vma=False,
    )
```
